32 devices in a mesh: blk: 8 (over y, x, core), grp: 4 (over z).
Axes of the slice: x: 2, y: 2, z: 4, core: 2. Of those that a mesh axis runs over, the one named last changes fastest.
Arguments:
- image_tokens: float32 [128, 49, 256], P(('blk', 'grp')), may hold values from -256 to 256
- text_tokens: float32 [128, 32, 256], P('blk'), may hold values from -4 to 4
- labels: int32 [128], P(('blk', 'grp')), may hold values from 0 to 127, each once
Outputs:
- loss_total: float32 [], replicated
- image_grads: float32 [128, 49, 256], P(('blk', 'grp'))
- text_grads: float32 [128, 32, 256], P('blk')
The draws below stay inside these ranges and needn't reach their ends.
Inputs may be any that keep to these rules, and one draw needn't show every extreme that they name: `labels`: each text index appears exactly once.
All inputs are finite; a program needn't handle non-finite values.
Results may differ from the reference program's by a relative error of at most 0.0003.
Values sent between devices are 32-bit elements; how exact they have to be, the bound alone decides.
No kernel may reach another device: no remote copies, remote signals or barrier semaphores. Data moves between devices by JAX's collectives and lax.ppermute only.
A program may use at most 128 MiB of HBM per device.

```python
import jax
import jax.numpy as jnp
from jax import lax

D = 256
NI = 49
NT = 32
B_DEV = 4
IMAGES = 128
TEXTS = 128


def text_common(key):
    noise_key = jax.random.fold_in(key, 0)
    base = jnp.clip(jax.random.normal(noise_key, (TEXTS, NT, D), jnp.float32) * 0.3, -1.8, 1.8)
    return base


def draw_text_tokens(key, part):
    return text_common(jax.random.fold_in(key, 11))


def draw_image_tokens(key, part):
    own_key = jax.random.fold_in(key, 12)
    noise_key = jax.random.fold_in(own_key, 0)
    base = jnp.clip(jax.random.normal(noise_key, (IMAGES, NI, D), jnp.float32) * 0.3, -1.8, 1.8)
    return base


def setup_inputs(seed: int = 0) -> dict:
    key_list = jax.random.split(jax.random.key(seed), 4)
    return {
        "image_tokens": draw_image_tokens(jax.random.fold_in(key_list[3], 71), 0),
        "text_tokens": draw_text_tokens(jax.random.fold_in(key_list[3], 71), 0),
        "labels": jax.random.permutation(key_list[2], IMAGES).astype(jnp.int32),
    }


HIGH = lax.Precision.HIGHEST


def pair_terms(images, texts, labels, text_start):
    scores = jnp.einsum("bid,cjd->ijbc", images, texts, precision=HIGH)
    row_max = jnp.max(scores, axis=1, keepdims=True)
    row_exp = jnp.exp(scores - row_max)
    row_sum = jnp.sum(row_exp, axis=1, keepdims=True)
    col_max = jnp.max(scores, axis=0, keepdims=True)
    col_exp = jnp.exp(scores - col_max)
    col_sum = jnp.sum(col_exp, axis=0, keepdims=True)
    image_pool = row_max[:, 0] + jnp.log(row_sum[:, 0])
    text_pool = col_max[0] + jnp.log(col_sum[0])
    pair = 0.5 * (jnp.mean(image_pool, axis=0) + jnp.mean(text_pool, axis=0))
    logit = 4.0 * pair - 20.0
    columns = text_start + jnp.arange(texts.shape[0], dtype=jnp.int32)
    sign = jnp.where(labels[:, None] == columns[None, :], 1.0, -1.0).astype(logit.dtype)
    summed = jnp.sum(jax.nn.softplus(-sign * logit))
    dpair = -2.0 * sign * jax.nn.sigmoid(-sign * logit)
    weights = row_exp / row_sum / images.shape[1] + col_exp / col_sum / texts.shape[1]
    dscore = 0.5 * dpair[None, None] * weights
    dimage = jnp.einsum("ijbc,cjd->bid", dscore, texts, precision=HIGH)
    dtext = jnp.einsum("ijbc,bid->cjd", dscore, images, precision=HIGH)
    return summed, dimage, dtext


def reference(image_tokens, text_tokens, labels):
    blocks = image_tokens.reshape(IMAGES // B_DEV, B_DEV, NI, D)
    label_blocks = labels.reshape(IMAGES // B_DEV, B_DEV)

    def step(carry, inputs):
        summed, dimage, dtext = pair_terms(inputs[0], text_tokens, inputs[1], 0)
        return (carry[0] + summed, carry[1] + dtext), dimage

    start = (jnp.zeros((), jnp.float32), jnp.zeros((TEXTS, NT, D), jnp.float32))
    (summed, text_grads), image_blocks = lax.scan(step, start, (blocks, label_blocks))
    return summed / IMAGES, image_blocks.reshape(IMAGES, NI, D), text_grads
```

```python
import functools

import jax
import jax.numpy as jnp
from jax import lax
from jax.experimental import pallas as pl
from jax.experimental.pallas import tpu as pltpu
from jax.sharding import PartitionSpec as P


F32 = jnp.float32
BF16 = jnp.bfloat16
LOW = -1e30


def swap(x, axis, k):
    n = lax.axis_size(axis)
    return lax.ppermute(x, axis, [(i, i ^ k) for i in range(n)])


def split(x, parts):
    out = []
    for p in range(parts):
        h = x.astype(BF16)
        out.append(h)
        if p + 1 < parts:
            x = x - h.astype(F32)
    return out


def dot_nt(a, b):
    return lax.dot_general(a, b, (((1,), (1,)), ((), ())), preferred_element_type=F32)


def dot_nn(a, b):
    return lax.dot_general(a, b, (((1,), (0,)), ((), ())), preferred_element_type=F32)


def lane_all(x, op, step):
    while step < 128:
        x = op(x, pltpu.roll(x, step, 1))
        step *= 2
    return x


def sublane_all(x, op, step):
    while step < 8:
        x = op(x, pltpu.roll(x, step, 0))
        step *= 2
    return x


def piece_kernel(dims, last, lab_ref, start_ref, img_ref, ta_ref, tb_ref, *refs):
    ni, nb, nt, nc, d = dims
    if len(refs) == 10:
        acc_in, refs = refs[:3], refs[3:]
    else:
        acc_in = None
    dimg_ref, acca_ref, accb_ref, loss_ref, i_scr, di_scr, o_scr = refs
    rows = ni * nb
    tiles = -(-rows // 8)
    rp = tiles * 8
    width = nt * nc
    left = rows - (tiles - 1) * 8

    if rp != rows:
        i_scr[rp - 8 :, :] = jnp.zeros((8, d), F32)
    for i in range(ni):
        i_scr[i * nb : (i + 1) * nb, :] = img_ref[i]
    img = i_scr[...]
    ih, im, il = split(img, 3)
    it = img.T
    ith, itl = split(it, 2)

    sub = lax.broadcasted_iota(jnp.int32, (8, 128), 0)
    lane = lax.broadcasted_iota(jnp.int32, (8, 128), 1)
    lab = jnp.zeros((8, 128), jnp.int32)
    for b in range(nb):
        lab = jnp.where(sub % nb == b, lab_ref[b], lab)
    pad_row = lax.broadcasted_iota(jnp.int32, (8, 1), 0) >= left

    loss = jnp.zeros((8, 128), F32)
    for half, t_ref in enumerate((ta_ref, tb_ref)):
        texts = []
        for k in range(0, d, 128):
            o_scr[...] = t_ref[:, k : k + 128]
            texts.append(
                jnp.concatenate(
                    [o_scr[pl.ds(j, nc, stride=nt), :] for j in range(nt)], axis=0
                )
            )
        th, tm, tl = split(jnp.concatenate(texts, axis=1), 3)
        s = (
            dot_nt(ih, th)
            + (dot_nt(ih, tm) + dot_nt(im, th))
            + (dot_nt(im, tm) + dot_nt(ih, tl) + dot_nt(il, th))
        )
        if rp != rows:
            s = jnp.concatenate(
                [s[: rp - 8], jnp.where(pad_row, LOW, s[rp - 8 :])], axis=0
            )
        cols = [s[:, k : k + 128] for k in range(0, width, 128)]
        row_max = lane_all(functools.reduce(jnp.maximum, cols), jnp.maximum, nc)
        row_exp = [jnp.exp(x - row_max) for x in cols]
        row_sum = lane_all(functools.reduce(jnp.add, row_exp), jnp.add, nc)
        image_pool = (row_max + jnp.log(row_sum)).reshape(tiles, 8, 128)
        pooled = jnp.sum(image_pool[: tiles - 1], axis=0) + jnp.where(
            pad_row, 0.0, image_pool[tiles - 1]
        )
        pooled = sublane_all(pooled, jnp.add, nb) * (1.0 / ni)
        col_exp, col_sum, texts_pooled = [], [], jnp.zeros((8, 128), F32)
        for x in cols:
            x3 = x.reshape(tiles, 8, 128)
            m = sublane_all(jnp.max(x3, axis=0), jnp.maximum, nb)
            e = jnp.exp(x3 - m[None])
            z = sublane_all(jnp.sum(e, axis=0), jnp.add, nb)
            col_exp.append(e)
            col_sum.append(z)
            texts_pooled = texts_pooled + (m + jnp.log(z))
        texts_pooled = lane_all(texts_pooled, jnp.add, nc) * (1.0 / nt)
        logit = 4.0 * (0.5 * (pooled + texts_pooled)) - 20.0
        sign = jnp.where(lab == start_ref[half] + lane % nc, 1.0, -1.0)
        z = -sign * logit
        e = jnp.exp(-jnp.abs(z))
        loss = loss + (jnp.maximum(z, 0.0) + jnp.log1p(e))
        sig = jnp.where(z >= 0.0, 1.0, e) / (1.0 + e)
        dpair = -2.0 * sign * sig
        row_w = (0.5 / ni) * dpair[None] / row_sum.reshape(tiles, 8, 128)
        if rp != rows:
            row_w = jnp.concatenate(
                [row_w[: tiles - 1], jnp.where(pad_row, 0.0, row_w[tiles - 1])[None]],
                axis=0,
            )
        ds = [
            (
                re.reshape(tiles, 8, 128) * row_w
                + ce * ((0.5 / nt) * dpair / cz)[None]
            ).reshape(rp, 128)
            for re, ce, cz in zip(row_exp, col_exp, col_sum)
        ]
        wh, wl = split(jnp.concatenate(ds, axis=1), 2)
        di = dot_nn(wh, th) + (dot_nn(wh, tm) + dot_nn(wl, th))
        if half == 0:
            di_scr[...] = di
        else:
            di_scr[...] += di
        dt = dot_nn(ith, wh) + (dot_nn(ith, wl) + dot_nn(itl, wh))
        if acc_in is not None:
            dt = dt + acc_in[half][...]
        out = (acca_ref, accb_ref)[half]
        if last:
            turned = dt.T
            for k in range(0, d, 128):
                for j in range(nt):
                    o_scr[pl.ds(j, nc, stride=nt), :] = turned[
                        j * nc : (j + 1) * nc, k : k + 128
                    ]
                out[:, k : k + 128] = o_scr[...]
        else:
            out[...] = dt
    for i in range(ni):
        dimg_ref[i] = di_scr[i * nb : (i + 1) * nb, :]
    loss = loss * (1.0 / ((8 // nb) * (128 // nc)))
    if acc_in is not None:
        loss = loss + acc_in[2][...]
    loss_ref[...] = loss


def piece(img, lab, starts, ta, tb, acc, last, dims):
    ni, nb, nt, nc, d = dims
    rp = -(-(ni * nb) // 8) * 8
    width = nt * nc
    smem = pl.BlockSpec(memory_space=pltpu.SMEM)
    vmem = pl.BlockSpec(memory_space=pltpu.VMEM)
    acc_shape = (width, d) if last else (d, width)
    flops = 2 * ni * nb * 2 * width * d * 12
    return pl.pallas_call(
        functools.partial(piece_kernel, dims, last),
        out_shape=(
            jax.ShapeDtypeStruct((ni, nb, d), F32),
            jax.ShapeDtypeStruct(acc_shape, F32),
            jax.ShapeDtypeStruct(acc_shape, F32),
            jax.ShapeDtypeStruct((8, 128), F32),
        ),
        in_specs=[smem, smem] + [vmem] * (3 + len(acc)),
        out_specs=(vmem,) * 4,
        scratch_shapes=[
            pltpu.VMEM((rp, d), F32),
            pltpu.VMEM((rp, d), F32),
            pltpu.VMEM((width, 128), F32),
        ],
        cost_estimate=pl.CostEstimate(
            flops=flops, bytes_accessed=8 * width * d * 4, transcendentals=4 * ni * nb * width
        ),
        compiler_params=pltpu.CompilerParams(vmem_limit_bytes=48 * 1024 * 1024),
    )(lab, starts, img, ta, tb, *acc)


def on_device(image_tokens, text_tokens, labels):
    nb, ni, d = image_tokens.shape
    nc, nt, _ = text_tokens.shape
    n_blk, n_grp = lax.axis_size("blk"), lax.axis_size("grp")
    count = nb * n_blk * n_grp
    dims = (ni, nb, nt, nc, d)
    blk, grp = lax.axis_index("blk"), lax.axis_index("grp")

    mine = jnp.transpose(image_tokens, (1, 0, 2))
    texts = text_tokens.reshape(nc * nt, d)
    far = range(2, n_blk, 2)
    pieces = [(mine, labels)] + [
        (swap(mine, "blk", k), swap(labels, "blk", k)) for k in far
    ]
    other = swap(texts, "blk", 1)
    starts = jnp.stack([(blk ^ 1) * nc, blk * nc]).astype(jnp.int32)

    acc, grads = (), []
    for p, (img, lab) in enumerate(pieces):
        g, *acc = piece(img, lab, starts, other, texts, acc, p + 1 == len(pieces), dims)
        grads.append(g)
    acc_other, acc_mine, loss = acc

    shard = (acc_mine + swap(acc_other, "blk", 1)).reshape(n_grp, nc // n_grp, nt, d)
    order = sorted(range(1, n_grp), key=lambda k: -k)
    arrived = [
        swap(lax.dynamic_index_in_dim(shard, grp ^ k, 0, False), "grp", k) for k in order
    ]
    total = lax.dynamic_index_in_dim(shard, grp, 0, False)
    for a in arrived:
        total = total + a
    whole = shard
    for k, a in [(k, swap(total, "grp", k)) for k in order] + [(0, total)]:
        whole = lax.dynamic_update_index_in_dim(whole, a, grp ^ k, 0)
    text_grads = whole.reshape(nc, nt, d)

    image_grads = grads[0]
    for k, g in zip(far, grads[1:]):
        image_grads = image_grads + swap(g, "blk", k)
    image_grads = jnp.transpose(image_grads, (1, 0, 2))

    for axis, n in (("blk", n_blk), ("grp", n_grp)):
        k = 1
        while k < n:
            loss = loss + swap(loss, axis, k)
            k *= 2
    return jnp.sum(loss) / count, image_grads, text_grads


def solution(mesh):
    placed = (P(("blk", "grp"), None, None), P("blk", None, None), P(("blk", "grp")))
    return jax.shard_map(
        on_device,
        mesh=mesh,
        in_specs=placed,
        out_specs=(P(), P(("blk", "grp"), None, None), P("blk", None, None)),
        check_vma=False,
    )
```

```python
import functools

import jax
import jax.numpy as jnp
from jax import lax
from jax.experimental import pallas as pl
from jax.experimental.pallas import tpu as pltpu
from jax.sharding import PartitionSpec as P


F32 = jnp.float32
BF16 = jnp.bfloat16
LOW = -1e30
LOG2E = 1.4426950408889634
LN2 = 0.6931471805599453


def swap(x, axis, k):
    n = lax.axis_size(axis)
    return lax.ppermute(x, axis, [(i, i ^ k) for i in range(n)])


def tree_sum(values):
    while len(values) > 1:
        values = [a + b for a, b in zip(values[::2], values[1::2])]
    return values[0]


def split(x, parts):
    out = []
    for p in range(parts):
        h = x.astype(BF16)
        out.append(h)
        if p + 1 < parts:
            x = x - h.astype(F32)
    return out


def dot_nt(a, b):
    return lax.dot_general(a, b, (((1,), (1,)), ((), ())), preferred_element_type=F32)


def dot_nn(a, b):
    return lax.dot_general(a, b, (((1,), (0,)), ((), ())), preferred_element_type=F32)


def lane_all(x, op, step):
    while step < 128:
        x = op(x, pltpu.roll(x, step, 1))
        step *= 2
    return x


def sublane_all(x, op, step):
    while step < 8:
        x = op(x, pltpu.roll(x, step, 0))
        step *= 2
    return x


def scores_of(img, t_parts):
    ih, im, il = img
    th, tm, tl = t_parts
    return (
        dot_nt(ih, th)
        + (dot_nt(ih, tm) + dot_nt(im, th))
        + (dot_nt(im, tm) + dot_nt(ih, tl) + dot_nt(il, th))
    )


def pair_math(dims, s, lab, text):
    ni, nb, nt, nc, _ = dims
    rows, (rp, width) = ni * nb, s.shape
    tiles = rp // 8
    pad = lax.broadcasted_iota(jnp.int32, (8, 1), 0) >= rows - 8 * (tiles - 1)

    def on_last(x, fill):
        if rp == rows:
            return x
        return jnp.concatenate(
            [x[: tiles - 1], jnp.where(pad, fill, x[tiles - 1])[None]], axis=0
        )

    cols = [
        on_last((s[:, k : k + 128] * LOG2E).reshape(tiles, 8, 128), LOW)
        for k in range(0, width, 128)
    ]

    def over_lanes(x, op):
        return lane_all(x.reshape(rp, 128), op, nc).reshape(tiles, 8, 128)

    row_max = over_lanes(functools.reduce(jnp.maximum, cols), jnp.maximum)
    col_max = [sublane_all(jnp.max(x, axis=0), jnp.maximum, nb) for x in cols]
    row_exp = [jnp.exp2(x - row_max) for x in cols]
    row_sum = over_lanes(functools.reduce(jnp.add, row_exp), jnp.add)
    col_exp = [jnp.exp2(x - m[None]) for x, m in zip(cols, col_max)]
    col_sum = [sublane_all(jnp.sum(x, axis=0), jnp.add, nb) for x in col_exp]
    image_pool = on_last(row_max * LN2 + jnp.log(row_sum), 0.0)
    image_pool = sublane_all(jnp.sum(image_pool, axis=0), jnp.add, nb) * (1.0 / ni)
    text_pool = functools.reduce(
        jnp.add, [m * LN2 + jnp.log(z) for m, z in zip(col_max, col_sum)]
    )
    text_pool = lane_all(text_pool, jnp.add, nc) * (1.0 / nt)
    logit = 4.0 * (0.5 * (image_pool + text_pool)) - 20.0
    sign = jnp.where(lab == text, 1.0, -1.0)
    z = -sign * logit
    e = jnp.exp(-jnp.abs(z))
    loss = jnp.maximum(z, 0.0) + jnp.log1p(e)
    dpair = -2.0 * sign * (jnp.where(z >= 0.0, 1.0, e) / (1.0 + e))
    row_w = on_last(((0.5 / ni) * dpair)[None] / row_sum, 0.0)
    ds = [
        (re * row_w + ce * ((0.5 / nt) * dpair / cz)[None]).reshape(rp, 128)
        for re, ce, cz in zip(row_exp, col_exp, col_sum)
    ]
    return jnp.concatenate(ds, axis=1), loss


def piece_kernel(dims, n_pieces, first, last, *refs):
    ni, nb, nt, nc, d = dims
    rows = ni * nb
    rp = -(-rows // 8) * 8
    half = nc // 2
    refs = list(refs)

    def take(n):
        out, refs[:] = refs[:n], refs[n:]
        return out

    (first_ref,) = take(1)
    labs, imgs = take(n_pieces), take(n_pieces)
    if first:
        texts = take(2)
    else:
        t_parts, (acc_in, loss_in) = take(3), take(2)
    dimgs = take(n_pieces)
    if last:
        acc_out, (loss_ref,) = take(2), take(1)
    else:
        acc_out, loss_ref = take(2)
    if first:
        t_parts = take(3)
    if first or last:
        o_scr = take(4)
    scrs = take(n_pieces)
    if first:
        lab_scr, img_scr, text_scr, sems = take(4)
        bring = [
            pltpu.make_async_copy(src, dst, sems.at[i])
            for i, (src, dst) in enumerate(
                [(texts[1], text_scr), (imgs[0], img_scr), (labs[0], lab_scr)]
            )
        ]
        for copy in bring:
            copy.start()
        labs, imgs = [lab_scr], [img_scr]

    if first:
        for h, t_ref in enumerate((texts[0], text_scr)):
            if h == 1:
                for copy in bring:
                    copy.wait()
            for k in range(0, d, 128):
                scr = o_scr[2 * h + k // 128]
                scr[...] = t_ref[:, k : k + 128]
        turned = jnp.concatenate(
            [
                jnp.concatenate(
                    [
                        o_scr[2 * h + k // 128][pl.ds(j, half, stride=nt), :]
                        for j in range(nt)
                        for h in range(2)
                    ],
                    axis=0,
                )
                for k in range(0, d, 128)
            ],
            axis=1,
        )
        for ref, x in zip(t_parts, split(turned, 3)):
            ref[...] = x
    tp = [ref[...] for ref in t_parts]

    img_parts, lab_tiles = [], []
    at = lax.broadcasted_iota(jnp.int32, (8, nb), 0) % nb
    pick = at == lax.broadcasted_iota(jnp.int32, (8, nb), 1)
    for scr, img_ref, lab_ref in zip(scrs, imgs, labs):
        if rp != rows:
            scr[rp - 8 :, :] = jnp.zeros((8, d), F32)
        for i in range(ni):
            scr[i * nb : (i + 1) * nb, :] = img_ref[i]
        lab = jnp.broadcast_to(lab_ref[...].astype(F32), (8, nb))
        lab = jnp.sum(jnp.where(pick, lab, 0.0), axis=1, keepdims=True)
        lab_tiles.append(lab.astype(jnp.int32))

    loss = jnp.zeros((8, 128), F32)
    acc = None if first else acc_in[...]
    scores = []
    for scr in scrs:
        parts = split(scr[...], 3)
        img_parts.append(split(scr[...].T, 2))
        scores.append(scores_of(parts, tp))
    for p in range(n_pieces):
        ds, piece_loss = pair_math(dims, scores[p], lab_tiles[p], first_ref[...])
        loss = loss + piece_loss
        wh, wl = split(ds, 2)
        th, tm, _ = tp
        dimgs[p][...] = dot_nn(wh, th) + (dot_nn(wh, tm) + dot_nn(wl, th))
        ith, itl = img_parts[p]
        dt = dot_nn(ith, wh) + (dot_nn(ith, wl) + dot_nn(itl, wh))
        acc = dt if acc is None else acc + dt
    loss = loss * (1.0 / ((8 // nb) * (128 // nc)))
    loss = loss if first else loss + loss_in[...]
    loss_ref[...] = loss
    if last:
        acc_out[0][nt * half :, :128] = loss
        acc_out[0][nt * half :, 128:] = jnp.zeros((8, d - 128), F32)
        turned = acc.T
        for h in range(2):
            for k in range(0, d, 128):
                scr = o_scr[2 * h + k // 128]
                for j in range(nt):
                    at = j * nc + h * half
                    scr[pl.ds(j, half, stride=nt), :] = turned[at : at + half, k : k + 128]
                acc_out[h][: nt * half, k : k + 128] = scr[...]
    else:
        acc_out[...] = acc


def stay(x):
    return pltpu.with_memory_space_constraint(x, pltpu.HBM)


def pieces_call(dims, text_ids, labs, imgs, texts, state, last):
    ni, nb, nt, nc, d = dims
    rp = -(-(ni * nb) // 8) * 8
    width = nt * nc
    n = len(imgs)
    first = state is None
    vmem = pl.BlockSpec(memory_space=pltpu.VMEM)
    shape = jax.ShapeDtypeStruct
    args = list(texts) if first else list(state)
    specs = [vmem] * (1 + 2 * n + len(args))
    if first:
        for at in (1, 2, 4):
            specs[at] = pl.BlockSpec(memory_space=pltpu.HBM)
        labs, imgs, args[1] = (
            [stay(labs[0])], [stay(imgs[0])], stay(args[1])
        )
    outs = [shape((rp, d), F32)] * n
    if last:
        outs += [shape((width // 2 + 8, d), F32), shape((width // 2, d), F32)]
    else:
        outs += [shape((d, width), F32)]
    outs += [shape((8, 128), F32)]
    outs += [shape((width, d), BF16)] * 3 if first else []
    scratch = [pltpu.VMEM((width // 2, 128), F32)] * 4 if first or last else []
    scratch += [pltpu.VMEM((rp, d), F32)] * n
    if first:
        scratch += [
            pltpu.VMEM((1, nb), jnp.int32),
            pltpu.VMEM((ni, nb, d), F32),
            pltpu.VMEM((width // 2, d), F32),
            pltpu.SemaphoreType.DMA((3,)),
        ]
    out = pl.pallas_call(
        functools.partial(piece_kernel, dims, n, first, last),
        out_shape=tuple(outs),
        in_specs=specs,
        out_specs=(vmem,) * len(outs),
        scratch_shapes=scratch,
        cost_estimate=pl.CostEstimate(
            flops=2 * ni * nb * width * d * 12 * n,
            bytes_accessed=8 * width * d * 4,
            transcendentals=2 * ni * nb * width * n,
        ),
        compiler_params=pltpu.CompilerParams(vmem_limit_bytes=48 * 1024 * 1024),
    )(text_ids, *labs, *imgs, *args)
    return list(out[:n]), list(out[n:])


def sum_kernel(n, *refs):
    out_ref = refs[n]
    ni, nb, _ = out_ref.shape
    for i in range(ni):
        at = slice(i * nb, (i + 1) * nb)
        out_ref[i] = tree_sum([ref[at, :] for ref in refs[:n]])


def sum_pieces(pieces, ni, nb):
    d = pieces[0].shape[1]
    return pl.pallas_call(
        functools.partial(sum_kernel, len(pieces)),
        out_shape=jax.ShapeDtypeStruct((ni, nb, d), F32),
        in_specs=[pl.BlockSpec(memory_space=pltpu.VMEM)] * len(pieces),
        out_specs=pl.BlockSpec(memory_space=pltpu.VMEM),
        compiler_params=pltpu.CompilerParams(vmem_limit_bytes=16 * 1024 * 1024),
    )(*pieces)


def CUTS(n):
    return [0, 1, 2, n]


def steps(image_tokens, text_tokens, labels):
    nb, ni, d = image_tokens.shape
    nc, nt, _ = text_tokens.shape
    n_blk, n_grp = lax.axis_size("blk"), lax.axis_size("grp")
    count = nb * n_blk * n_grp
    dims = (ni, nb, nt, 2 * nc, d)
    blk, grp = lax.axis_index("blk"), lax.axis_index("grp")
    far = list(range(2, n_blk, 2))
    order = grp_order(n_grp)

    mine = jnp.transpose(image_tokens, (1, 0, 2))
    labels = labels.reshape(1, nb)
    texts = text_tokens.reshape(nc * nt, d)
    imgs = [mine] + [swap(mine, "blk", k) for k in far]
    labs = [labels] + [swap(labels, "blk", k) for k in far]
    other = swap(texts, "blk", 1)
    lane = lax.broadcasted_iota(jnp.int32, (8, 128), 1) % (2 * nc)
    text_ids = lane % nc + nc * jnp.where(lane < nc, blk ^ 1, blk)

    state, t_parts, grads = None, None, []
    cuts = CUTS(len(imgs))
    for lo, hi in zip(cuts[:-1], cuts[1:]):
        last = hi == len(imgs)
        g, out = pieces_call(dims, text_ids, labs[lo:hi], imgs[lo:hi], (other, texts), state, last)
        grads += g
        if state is None and not last:
            t_parts = out[2:]
        state = (*t_parts, *out[:2]) if not last else out
    acc_other, acc_mine, loss = state

    recv = swap(acc_other, "blk", 1)
    shard = (acc_mine + recv[: nc * nt]).reshape(n_grp, nc // n_grp, nt, d)
    loss = loss + recv[nc * nt :, :128]
    arrived = [
        swap(lax.dynamic_index_in_dim(shard, grp ^ k, 0, False), "grp", k)
        for k in order
    ]
    total = lax.dynamic_index_in_dim(shard, grp, 0, False)
    for a in arrived:
        total = total + a
    whole = shard
    for k, a in [(k, swap(total, "grp", k)) for k in order] + [(0, total)]:
        whole = lax.dynamic_update_index_in_dim(whole, a, grp ^ k, 0)
    text_grads = whole.reshape(nc, nt, d)

    grads = grads[:1] + [swap(g, "blk", k) for k, g in zip(far, grads[1:])]
    image_grads = jnp.transpose(sum_pieces(grads, ni, nb), (1, 0, 2))

    loss = tree_sum([loss] + [swap(loss, "blk", k) for k in far])
    loss = tree_sum([loss] + [swap(loss, "grp", k) for k in range(1, n_grp)])
    return jnp.sum(loss) / count, image_grads, text_grads


def grp_order(n_grp):
    return sorted(range(1, n_grp), key=lambda k: -k)


def solution(mesh):
    placed = (P(("blk", "grp"), None, None), P("blk", None, None), P(("blk", "grp")))
    return jax.shard_map(
        steps,
        mesh=mesh,
        in_specs=placed,
        out_specs=(P(), P(("blk", "grp"), None, None), P("blk", None, None)),
        check_vma=False,
    )
```

```python
import functools

import jax
import jax.numpy as jnp
from jax import lax
from jax.experimental import pallas as pl
from jax.experimental.pallas import tpu as pltpu
from jax.sharding import PartitionSpec as P


F32 = jnp.float32
BF16 = jnp.bfloat16
LOW = -1e30
LOG2E = 1.4426950408889634
LN2 = 0.6931471805599453
MIB = 1024 * 1024


def ORDER(n):
    return sorted(range(1, n), key=lambda k: -k)


def swap(x, axis, k):
    n = lax.axis_size(axis)
    return lax.ppermute(x, axis, [(i, i ^ k) for i in range(n)])


def tree_sum(values):
    while len(values) > 1:
        values = [a + b for a, b in zip(values[::2], values[1::2])]
    return values[0]


def split(x, parts):
    out = []
    for p in range(parts):
        h = x.astype(BF16)
        out.append(h)
        if p + 1 < parts:
            x = x - h.astype(F32)
    return out


def dot_nt(a, b):
    return lax.dot_general(a, b, (((1,), (1,)), ((), ())), preferred_element_type=F32)


def dot_nn(a, b):
    return lax.dot_general(a, b, (((1,), (0,)), ((), ())), preferred_element_type=F32)


def lane_all(x, op, step):
    while step < 128:
        x = op(x, pltpu.roll(x, step, 1))
        step *= 2
    return x


def sublane_all(x, op, step):
    while step < 8:
        x = op(x, pltpu.roll(x, step, 0))
        step *= 2
    return x


def stay(x):
    return pltpu.with_memory_space_constraint(x, pltpu.HBM)


def specs(n):
    return [pl.BlockSpec(memory_space=pltpu.VMEM)] * n


def scores_of(img, t_parts):
    ih, im, il = img
    th, tm, tl = t_parts
    return (
        dot_nt(ih, th)
        + (dot_nt(ih, tm) + dot_nt(im, th))
        + (dot_nt(im, tm) + dot_nt(ih, tl) + dot_nt(il, th))
    )


def pair_math(dims, s, lab, text):
    ni, nb, nt, nc, _ = dims
    rows, (rp, width) = ni * nb, s.shape
    tiles = rp // 8
    pad = lax.broadcasted_iota(jnp.int32, (8, 1), 0) >= rows - 8 * (tiles - 1)

    def on_last(x, fill):
        if rp == rows:
            return x
        return jnp.concatenate(
            [x[: tiles - 1], jnp.where(pad, fill, x[tiles - 1])[None]], axis=0
        )

    cols = [
        on_last((s[:, k : k + 128] * LOG2E).reshape(tiles, 8, 128), LOW)
        for k in range(0, width, 128)
    ]

    def over_lanes(x, op):
        return lane_all(x.reshape(rp, 128), op, nc).reshape(tiles, 8, 128)

    row_max = over_lanes(functools.reduce(jnp.maximum, cols), jnp.maximum)
    col_max = [sublane_all(jnp.max(x, axis=0), jnp.maximum, nb) for x in cols]
    row_exp = [jnp.exp2(x - row_max) for x in cols]
    row_sum = over_lanes(functools.reduce(jnp.add, row_exp), jnp.add)
    col_exp = [jnp.exp2(x - m[None]) for x, m in zip(cols, col_max)]
    col_sum = [sublane_all(jnp.sum(x, axis=0), jnp.add, nb) for x in col_exp]
    image_pool = on_last(row_max * LN2 + jnp.log(row_sum), 0.0)
    image_pool = sublane_all(jnp.sum(image_pool, axis=0), jnp.add, nb) * (1.0 / ni)
    text_pool = functools.reduce(
        jnp.add, [m * LN2 + jnp.log(z) for m, z in zip(col_max, col_sum)]
    )
    text_pool = lane_all(text_pool, jnp.add, nc) * (1.0 / nt)
    logit = 4.0 * (0.5 * (image_pool + text_pool)) - 20.0
    sign = jnp.where(lab == text, 1.0, -1.0)
    z = -sign * logit
    e = jnp.exp(-jnp.abs(z))
    loss = jnp.maximum(z, 0.0) + jnp.log1p(e)
    dpair = -2.0 * sign * (jnp.where(z >= 0.0, 1.0, e) / (1.0 + e))
    row_w = on_last(((0.5 / ni) * dpair)[None] / row_sum, 0.0)
    ds = [
        (re * row_w + ce * ((0.5 / nt) * dpair / cz)[None]).reshape(rp, 128)
        for re, ce, cz in zip(row_exp, col_exp, col_sum)
    ]
    return jnp.concatenate(ds, axis=1), loss * (1.0 / ((8 // nb) * (128 // nc)))


def label_tile(img_ref, nb):
    rp = img_ref.shape[0]
    tail = img_ref[rp - 8 :, :128]
    sub = lax.broadcasted_iota(jnp.int32, (8, 128), 0)
    return jnp.where(sub >= 8 - nb, tail, pltpu.roll(tail, nb, 0)).astype(jnp.int32)


def image_grad(w, t_parts):
    wh, wl = w
    th, tm, _ = t_parts
    return dot_nn(wh, th) + (dot_nn(wh, tm) + dot_nn(wl, th))


def text_grad(turned_img, w):
    (ith, itl), (wh, wl) = turned_img, w
    return dot_nn(ith, wh) + (dot_nn(ith, wl) + dot_nn(itl, wh))


def weights_of(dims, imgs, t_parts, text):
    scores, turned, out, losses = [], [], [], []
    for ref in imgs:
        img = ref[...]
        turned.append(split(img.T, 2))
        scores.append(scores_of(split(img, 3), t_parts))
    for ref, s in zip(imgs, scores):
        ds, loss = pair_math(dims, s, label_tile(ref, dims[1]), text)
        out.append(split(ds, 2))
        losses.append(loss)
    return turned, out, functools.reduce(jnp.add, losses)


def first_kernel(dims, ids_ref, img_ref, other_ref, own_ref, *refs):
    _, _, nt, nc, _ = dims
    half = nc // 2
    dimg_ref, acc_ref, loss_ref, *t_refs = refs[:6]
    scrs = refs[6:]
    for k, scr in enumerate(scrs):
        scr[...] = other_ref[:, 128 * k : 128 * (k + 1)]
    text = jnp.concatenate(
        [
            jnp.concatenate(
                [
                    x
                    for j in range(nt)
                    for x in (
                        scr[pl.ds(j, half, stride=nt), :],
                        own_ref[j * half : (j + 1) * half, 128 * k : 128 * (k + 1)],
                    )
                ],
                axis=0,
            )
            for k, scr in enumerate(scrs)
        ],
        axis=1,
    )
    for ref, x in zip(t_refs, split(text, 3)):
        ref[...] = x
    tp = [ref[...] for ref in t_refs]
    turned, w, loss = weights_of(dims, [img_ref], tp, ids_ref[...])
    loss_ref[...] = loss
    dimg_ref[...] = image_grad(w[0], tp)
    acc_ref[...] = text_grad(turned[0], w[0])


def middle_kernel(dims, n, ids_ref, *refs):
    imgs, (acc_in, loss_in, *t_refs) = refs[:n], refs[n : n + 5]
    dimgs, (acc_ref, loss_ref) = refs[n + 5 : 2 * n + 5], refs[2 * n + 5 :]
    tp = [ref[...] for ref in t_refs]
    turned, w, loss = weights_of(dims, imgs, tp, ids_ref[...])
    loss_ref[...] = loss_in[...] + loss
    acc = acc_in[...]
    for p in range(n):
        dimgs[p][...] = image_grad(w[p], tp)
        acc = acc + text_grad(turned[p], w[p])
    acc_ref[...] = acc


def hand_out(dims, turned, send_ref, own_ref):
    nt, nc, d = dims[2:]
    half = nc // 2
    for j in range(nt):
        g, q = divmod(j, 8)
        for k in range(d // 128):
            to = ((g * (d // 128) + k) * 8 + q) * half
            for h, ref in enumerate((send_ref, own_ref)):
                ref[to : to + half, :] = turned[
                    j * nc + h * half : j * nc + (h + 1) * half,
                    128 * k : 128 * (k + 1),
                ]


def last_kernel(dims, n, ids_ref, *refs):
    imgs, (acc_in, loss_in, *t_refs) = refs[:n], refs[n : n + 5]
    send_ref, own_ref, *keep = refs[n + 5 :]
    tp = [ref[...] for ref in t_refs]
    turned, w, loss = weights_of(dims, imgs, tp, ids_ref[...])
    acc = acc_in[...]
    for p in range(n):
        acc = acc + text_grad(turned[p], w[p])
        for ref, x in zip(keep[2 * p : 2 * p + 2], w[p]):
            ref[...] = x
    hand_out(dims, acc.T, send_ref, own_ref)
    for ref in (send_ref, own_ref):
        ref[ref.shape[0] - 8 :, :] = loss_in[...] + loss


def rest_kernel(n, th_ref, tm_ref, *refs):
    tp = (th_ref[...], tm_ref[...], None)
    for p in range(n):
        w = [ref[...] for ref in refs[2 * p : 2 * p + 2]]
        refs[2 * n + p][...] = image_grad(w, tp)


def call(kernel, outs, args, dims, n, mats, scratch=(), limit=48):
    ni, nb, nt, nc, d = dims
    return pl.pallas_call(
        kernel,
        out_shape=tuple(jax.ShapeDtypeStruct(*o) for o in outs),
        in_specs=specs(len(args)),
        out_specs=tuple(specs(len(outs))),
        scratch_shapes=list(scratch),
        cost_estimate=pl.CostEstimate(
            flops=2 * ni * nb * nt * nc * d * mats * n,
            bytes_accessed=4 * nt * nc * d,
            transcendentals=2 * ni * nb * nt * nc * n,
        ),
        compiler_params=pltpu.CompilerParams(vmem_limit_bytes=limit * MIB),
    )(*args)


def compute(dims, ids, imgs, other, own):
    ni, nb, nt, nc, d = dims
    width = nt * nc
    rp = ni * nb + nb
    part = (nt * nc * d // 2 // 128 + 8, 128)
    img, acc, loss = ((rp, d), F32), ((d, width), F32), ((8, 128), F32)
    keep = [((rp, width), BF16)] * 2
    dimgs = []
    out = call(
        functools.partial(first_kernel, dims),
        [img, acc, loss] + [((width, d), BF16)] * 3,
        [ids, imgs[0], other, own],
        dims,
        1,
        12,
        [pltpu.VMEM((width // 2, 128), F32)] * (d // 128),
    )
    dimgs.append(out[0])
    state, t_parts = out[1:3], out[3:]
    n_last = 2 if len(imgs) > 2 else 1
    for p in range(1, len(imgs) - n_last):
        *g, a, b = call(
            functools.partial(middle_kernel, dims, 1),
            [img, acc, loss],
            [ids, imgs[p], *state, *t_parts],
            dims,
            1,
            12,
        )
        dimgs += g
        state = (a, b)
    send, own, *kept = call(
        functools.partial(last_kernel, dims, n_last),
        [(part, F32)] * 2 + keep * n_last,
        [ids, *imgs[-n_last:], *state, *t_parts],
        dims,
        n_last,
        9,
    )
    g = call(
        functools.partial(rest_kernel, n_last),
        [img] * n_last,
        [*t_parts[:2], *kept],
        dims,
        n_last,
        3,
    )
    return dimgs + list(g), send, own


def pack_kernel(lab_hbm, img_hbm, out_ref, lab_scr, img_scr, sems):
    ni, nb, d = img_scr.shape
    bring = [
        pltpu.make_async_copy(img_hbm, img_scr, sems.at[0]),
        pltpu.make_async_copy(lab_hbm, lab_scr, sems.at[1]),
    ]
    for copy in bring:
        copy.start()
    for copy in bring:
        copy.wait()
    for i in range(ni):
        out_ref[i * nb : (i + 1) * nb, :] = img_scr[i]
    across = lax.broadcasted_iota(jnp.int32, (nb, nb), 0)
    along = lax.broadcasted_iota(jnp.int32, (nb, nb), 1)
    lab = jnp.broadcast_to(lab_scr[...].astype(F32), (nb, nb))
    lab = jnp.sum(jnp.where(across == along, lab, 0.0), axis=1, keepdims=True)
    out_ref[ni * nb :, :] = jnp.broadcast_to(lab, (nb, d))


def pack(images, labels):
    ni, nb, d = images.shape
    return pl.pallas_call(
        pack_kernel,
        out_shape=jax.ShapeDtypeStruct((ni * nb + nb, d), F32),
        in_specs=[pl.BlockSpec(memory_space=pltpu.HBM)] * 2,
        out_specs=pl.BlockSpec(memory_space=pltpu.VMEM),
        scratch_shapes=[
            pltpu.VMEM((1, nb), jnp.int32),
            pltpu.VMEM((ni, nb, d), F32),
            pltpu.SemaphoreType.DMA((2,)),
        ],
        compiler_params=pltpu.CompilerParams(vmem_limit_bytes=8 * MIB),
    )(stay(labels.reshape(1, nb)), stay(images))


def turn_kernel(nt, text_hbm, out_ref, *refs):
    *scrs, sems = refs
    half = scrs[0].shape[0] // nt
    bring = [
        pltpu.make_async_copy(
            text_hbm.at[:, pl.ds(128 * k, 128)], scr, sems.at[k]
        )
        for k, scr in enumerate(scrs)
    ]
    for copy in bring:
        copy.start()
    for k, scr in enumerate(scrs):
        bring[k].wait()
        for j in range(nt):
            out_ref[j * half : (j + 1) * half, 128 * k : 128 * (k + 1)] = scr[
                pl.ds(j, half, stride=nt), :
            ]


def turn(texts, nt):
    rows, d = texts.shape
    return pl.pallas_call(
        functools.partial(turn_kernel, nt),
        out_shape=jax.ShapeDtypeStruct((rows, d), F32),
        in_specs=[pl.BlockSpec(memory_space=pltpu.HBM)],
        out_specs=pl.BlockSpec(memory_space=pltpu.VMEM),
        scratch_shapes=[pltpu.VMEM((rows, 128), F32)] * (d // 128)
        + [pltpu.SemaphoreType.DMA((d // 128,))],
        compiler_params=pltpu.CompilerParams(vmem_limit_bytes=8 * MIB),
    )(stay(texts))


def sum_kernel(n, *refs):
    out_ref = refs[n]
    ni, nb, _ = out_ref.shape
    for i in range(ni):
        at = slice(i * nb, (i + 1) * nb)
        out_ref[i] = tree_sum([ref[at, :] for ref in refs[:n]])


def sum_pieces(pieces, ni, nb):
    d = pieces[0].shape[1]
    return pl.pallas_call(
        functools.partial(sum_kernel, len(pieces)),
        out_shape=jax.ShapeDtypeStruct((ni, nb, d), F32),
        in_specs=specs(len(pieces)),
        out_specs=specs(1)[0],
        compiler_params=pltpu.CompilerParams(vmem_limit_bytes=16 * MIB),
    )(*pieces)


def merge_kernel(n, own_ref, recv_ref, *outs):
    rows = outs[0].shape[0] - 8
    grp = lax.axis_index("grp")
    loss = own_ref[n * rows :, :] + recv_ref[n * rows :, :]
    for k, ref in enumerate(outs):
        at = pl.ds(pl.multiple_of((grp ^ k) * rows, 8), rows)
        ref[:rows, :] = own_ref[at, :] + recv_ref[at, :]
        ref[rows:, :] = loss


def merge(own, recv, n):
    rows = (own.shape[0] - 8) // n + 8
    return pl.pallas_call(
        functools.partial(merge_kernel, n),
        out_shape=(jax.ShapeDtypeStruct((rows, 128), F32),) * n,
        in_specs=specs(2),
        out_specs=tuple(specs(n)),
        compiler_params=pltpu.CompilerParams(vmem_limit_bytes=16 * MIB),
    )(own, recv)


def place_kernel(n, *refs):
    ranks, out_ref = refs[:n], refs[n]
    nc, nt, d = out_ref.shape
    lanes = d // 128
    units = nt // 8 * lanes // n
    grp = lax.axis_index("grp")
    for s in range(n):
        for i in range(units):
            unit = (grp ^ s) * units + i
            row = pl.multiple_of(8 * (unit // lanes), 8)
            lane = pl.multiple_of(128 * (unit % lanes), 128)
            for c in range(nc):
                out_ref[c, pl.ds(row, 8), pl.ds(lane, 128)] = ranks[s][
                    pl.ds(8 * nc * i + c, 8, stride=nc), :
                ]


def place(ranks, shape):
    return pl.pallas_call(
        functools.partial(place_kernel, len(ranks)),
        out_shape=jax.ShapeDtypeStruct(shape, F32),
        in_specs=specs(len(ranks)),
        out_specs=specs(1)[0],
        compiler_params=pltpu.CompilerParams(vmem_limit_bytes=16 * MIB),
    )(*ranks)


def steps(image_tokens, text_tokens, labels):
    nb, ni, d = image_tokens.shape
    nc, nt, _ = text_tokens.shape
    n_blk, n_grp = lax.axis_size("blk"), lax.axis_size("grp")
    count = nb * n_blk * n_grp
    dims = (ni, nb, nt, 2 * nc, d)
    blk = lax.axis_index("blk")
    far = list(range(2, n_blk, 2))
    order = grp_order(n_grp)

    mine = pack(jnp.transpose(image_tokens, (1, 0, 2)), labels)
    texts = text_tokens.reshape(nc * nt, d)
    imgs = [mine] + [swap(mine, "blk", k) for k in far]
    other = swap(texts, "blk", 1)
    own = turn(texts, nt)
    lane = lax.broadcasted_iota(jnp.int32, (8, 128), 1) % (2 * nc)
    text_ids = lane % nc + nc * jnp.where(lane < nc, blk ^ 1, blk)

    grads, send, own_part = compute(dims, text_ids, imgs, other, own)

    parts = merge(own_part, swap(send, "blk", 1), n_grp)
    arrived = {k: swap(parts[k], "grp", k) for k in order}
    total = tree_sum([parts[0]] + [arrived[k] for k in range(1, n_grp)])
    rows = total.shape[0] - 8
    total, loss = total[:rows], total[rows:]
    got = {k: swap(total, "grp", k) for k in order}
    text_grads = place([total] + [got[k] for k in range(1, n_grp)], (nc, nt, d))

    grads = grads[:1] + [swap(g, "blk", k) for k, g in zip(far, grads[1:])]
    image_grads = jnp.transpose(sum_pieces(grads, ni, nb), (1, 0, 2))

    parts = [loss] + [swap(loss, "blk", k) for k in far]
    loss = jnp.sum(tree_sum(parts)) / count
    return loss, image_grads, text_grads


def grp_order(n_grp):
    return ORDER(n_grp)


def solution(mesh):
    placed = (P(("blk", "grp"), None, None), P("blk", None, None), P(("blk", "grp")))
    return jax.shard_map(
        steps,
        mesh=mesh,
        in_specs=placed,
        out_specs=(P(), P(("blk", "grp"), None, None), P("blk", None, None)),
        check_vma=False,
    )
```

```python
import functools

import jax
import jax.numpy as jnp
from jax import lax
from jax.experimental import pallas as pl
from jax.experimental.pallas import tpu as pltpu
from jax.sharding import PartitionSpec as P


F32 = jnp.float32
BF16 = jnp.bfloat16
LOW = -1e30
LOG2E = 1.4426950408889634
LN2 = 0.6931471805599453
MIB = 1024 * 1024


def ORDER(n):
    first = [k for k in [3,2,1] if k < n]
    return first + [k for k in range(1, n) if k not in first]


def FAR(n):
    first = [k for k in [6,2,4] if k < n]
    return first + [k for k in range(2, n, 2) if k not in first]


def swap(x, axis, k):
    n = lax.axis_size(axis)
    return lax.ppermute(x, axis, [(i, i ^ k) for i in range(n)])


def tree_sum(values):
    while len(values) > 1:
        values = [a + b for a, b in zip(values[::2], values[1::2])]
    return values[0]


def split(x, parts):
    out = []
    for p in range(parts):
        h = x.astype(BF16)
        out.append(h)
        if p + 1 < parts:
            x = x - h.astype(F32)
    return out


def dot_nt(a, b):
    return lax.dot_general(a, b, (((1,), (1,)), ((), ())), preferred_element_type=F32)


def dot_nn(a, b):
    return lax.dot_general(a, b, (((1,), (0,)), ((), ())), preferred_element_type=F32)


def lane_all(x, op, step):
    while step < 128:
        x = op(x, pltpu.roll(x, step, 1))
        step *= 2
    return x


def sublane_all(x, op, step):
    while step < 8:
        x = op(x, pltpu.roll(x, step, 0))
        step *= 2
    return x


def stay(x):
    return pltpu.with_memory_space_constraint(x, pltpu.HBM)


def specs(n):
    return [pl.BlockSpec(memory_space=pltpu.VMEM)] * n


def scores_of(img, t_parts):
    ih, im, il = img
    th, tm, tl = t_parts
    return (
        dot_nt(ih, th)
        + (dot_nt(ih, tm) + dot_nt(im, th))
        + (dot_nt(im, tm) + dot_nt(ih, tl) + dot_nt(il, th))
    )


def pair_math(dims, s, lab, text):
    ni, nb, nt, nc, _ = dims
    rows, (rp, width) = ni * nb, s.shape
    tiles = rp // 8
    pad = lax.broadcasted_iota(jnp.int32, (8, 1), 0) >= rows - 8 * (tiles - 1)

    def on_last(x, fill):
        if rp == rows:
            return x
        return jnp.concatenate(
            [x[: tiles - 1], jnp.where(pad, fill, x[tiles - 1])[None]], axis=0
        )

    cols = [
        on_last((s[:, k : k + 128] * LOG2E).reshape(tiles, 8, 128), LOW)
        for k in range(0, width, 128)
    ]

    def over_lanes(x, op):
        return lane_all(x.reshape(rp, 128), op, nc).reshape(tiles, 8, 128)

    row_max = over_lanes(functools.reduce(jnp.maximum, cols), jnp.maximum)
    col_max = [sublane_all(jnp.max(x, axis=0), jnp.maximum, nb) for x in cols]
    row_exp = [jnp.exp2(x - row_max) for x in cols]
    row_sum = over_lanes(functools.reduce(jnp.add, row_exp), jnp.add)
    col_exp = [jnp.exp2(x - m[None]) for x, m in zip(cols, col_max)]
    col_sum = [sublane_all(jnp.sum(x, axis=0), jnp.add, nb) for x in col_exp]
    image_pool = on_last(row_max * LN2 + jnp.log(row_sum), 0.0)
    image_pool = sublane_all(jnp.sum(image_pool, axis=0), jnp.add, nb) * (1.0 / ni)
    text_pool = functools.reduce(
        jnp.add, [m * LN2 + jnp.log(z) for m, z in zip(col_max, col_sum)]
    )
    text_pool = lane_all(text_pool, jnp.add, nc) * (1.0 / nt)
    logit = 4.0 * (0.5 * (image_pool + text_pool)) - 20.0
    sign = jnp.where(lab == text, 1.0, -1.0)
    z = -sign * logit
    e = jnp.exp(-jnp.abs(z))
    loss = jnp.maximum(z, 0.0) + jnp.log1p(e)
    dpair = -2.0 * sign * (jnp.where(z >= 0.0, 1.0, e) / (1.0 + e))
    row_w = on_last(((0.5 / ni) * dpair)[None] / row_sum, 0.0)
    ds = [
        (re * row_w + ce * ((0.5 / nt) * dpair / cz)[None]).reshape(rp, 128)
        for re, ce, cz in zip(row_exp, col_exp, col_sum)
    ]
    return jnp.concatenate(ds, axis=1), loss * (1.0 / ((8 // nb) * (128 // nc)))


def label_tile(img_ref, nb):
    rp = img_ref.shape[0]
    tail = img_ref[rp - 8 :, :128]
    sub = lax.broadcasted_iota(jnp.int32, (8, 128), 0)
    return jnp.where(sub >= 8 - nb, tail, pltpu.roll(tail, nb, 0)).astype(jnp.int32)


def image_grad(w, t_parts):
    wh, wl = w
    th, tm, _ = t_parts
    return dot_nn(wh, th) + (dot_nn(wh, tm) + dot_nn(wl, th))


def text_grad(turned_img, w):
    (ith, itl), (wh, wl) = turned_img, w
    return dot_nn(ith, wh) + (dot_nn(ith, wl) + dot_nn(itl, wh))


def weights_of(dims, imgs, t_parts, text):
    scores, turned, out, losses = [], [], [], []
    for ref in imgs:
        img = ref[...]
        turned.append(split(img.T, 2))
        scores.append(scores_of(split(img, 3), t_parts))
    for ref, s in zip(imgs, scores):
        ds, loss = pair_math(dims, s, label_tile(ref, dims[1]), text)
        out.append(split(ds, 2))
        losses.append(loss)
    return turned, out, functools.reduce(jnp.add, losses)


def first_kernel(dims, ids_ref, img_ref, other_ref, own_ref, *refs):
    _, _, nt, nc, _ = dims
    half = nc // 2
    dimg_ref, acc_ref, loss_ref, *t_refs = refs[:6]
    scrs = refs[6:]
    for k, scr in enumerate(scrs):
        scr[...] = other_ref[:, 128 * k : 128 * (k + 1)]
    text = jnp.concatenate(
        [
            jnp.concatenate(
                [
                    x
                    for j in range(nt)
                    for x in (
                        scr[pl.ds(j, half, stride=nt), :],
                        own_ref[j * half : (j + 1) * half, 128 * k : 128 * (k + 1)],
                    )
                ],
                axis=0,
            )
            for k, scr in enumerate(scrs)
        ],
        axis=1,
    )
    for ref, x in zip(t_refs, split(text, 3)):
        ref[...] = x
    tp = [ref[...] for ref in t_refs]
    turned, w, loss = weights_of(dims, [img_ref], tp, ids_ref[...])
    loss_ref[...] = loss
    dimg_ref[...] = image_grad(w[0], tp)
    acc_ref[...] = text_grad(turned[0], w[0])


def middle_kernel(dims, n, ids_ref, *refs):
    imgs, (acc_in, loss_in, *t_refs) = refs[:n], refs[n : n + 5]
    dimgs, (acc_ref, loss_ref) = refs[n + 5 : 2 * n + 5], refs[2 * n + 5 :]
    tp = [ref[...] for ref in t_refs]
    turned, w, loss = weights_of(dims, imgs, tp, ids_ref[...])
    loss_ref[...] = loss_in[...] + loss
    acc = acc_in[...]
    for p in range(n):
        dimgs[p][...] = image_grad(w[p], tp)
        acc = acc + text_grad(turned[p], w[p])
    acc_ref[...] = acc


def hand_out(dims, turned, send_ref, own_ref):
    nt, nc, d = dims[2:]
    half = nc // 2
    for j in range(nt):
        g, q = divmod(j, 8)
        for k in range(d // 128):
            to = ((g * (d // 128) + k) * 8 + q) * half
            for h, ref in enumerate((send_ref, own_ref)):
                ref[to : to + half, :] = turned[
                    j * nc + h * half : j * nc + (h + 1) * half,
                    128 * k : 128 * (k + 1),
                ]


def last_kernel(dims, n, ids_ref, *refs):
    imgs, (acc_in, loss_in, *t_refs) = refs[:n], refs[n : n + 5]
    send_ref, own_ref, *keep = refs[n + 5 :]
    tp = [ref[...] for ref in t_refs]
    turned, w, loss = weights_of(dims, imgs, tp, ids_ref[...])
    acc = acc_in[...]
    for p in range(n):
        acc = acc + text_grad(turned[p], w[p])
        for ref, x in zip(keep[2 * p : 2 * p + 2], w[p]):
            ref[...] = x
    hand_out(dims, acc.T, send_ref, own_ref)
    for ref in (send_ref, own_ref):
        ref[ref.shape[0] - 8 :, :] = loss_in[...] + loss


def rest_kernel(n, th_ref, tm_ref, *refs):
    tp = (th_ref[...], tm_ref[...], None)
    for p in range(n):
        w = [ref[...] for ref in refs[2 * p : 2 * p + 2]]
        refs[2 * n + p][...] = image_grad(w, tp)


def call(kernel, outs, args, dims, n, mats, scratch=(), limit=48):
    ni, nb, nt, nc, d = dims
    return pl.pallas_call(
        kernel,
        out_shape=tuple(jax.ShapeDtypeStruct(*o) for o in outs),
        in_specs=specs(len(args)),
        out_specs=tuple(specs(len(outs))),
        scratch_shapes=list(scratch),
        cost_estimate=pl.CostEstimate(
            flops=2 * ni * nb * nt * nc * d * mats * n,
            bytes_accessed=4 * nt * nc * d,
            transcendentals=2 * ni * nb * nt * nc * n,
        ),
        compiler_params=pltpu.CompilerParams(vmem_limit_bytes=limit * MIB),
    )(*args)


def compute(dims, ids, imgs, other, own):
    ni, nb, nt, nc, d = dims
    width = nt * nc
    rp = ni * nb + nb
    part = (nt * nc * d // 2 // 128 + 8, 128)
    img, acc, loss = ((rp, d), F32), ((d, width), F32), ((8, 128), F32)
    keep = [((rp, width), BF16)] * 2
    dimgs = []
    out = call(
        functools.partial(first_kernel, dims),
        [img, acc, loss] + [((width, d), BF16)] * 3,
        [ids, imgs[0], other, own],
        dims,
        1,
        12,
        [pltpu.VMEM((width // 2, 128), F32)] * (d // 128),
    )
    dimgs.append(out[0])
    state, t_parts = out[1:3], out[3:]
    n_last = 2 if len(imgs) > 2 else 1
    for p in range(1, len(imgs) - n_last):
        *g, a, b = call(
            functools.partial(middle_kernel, dims, 1),
            [img, acc, loss],
            [ids, imgs[p], *state, *t_parts],
            dims,
            1,
            12,
        )
        dimgs += g
        state = (a, b)
    send, own, *kept = call(
        functools.partial(last_kernel, dims, n_last),
        [(part, F32)] * 2 + keep * n_last,
        [ids, *imgs[-n_last:], *state, *t_parts],
        dims,
        n_last,
        9,
    )
    g = call(
        functools.partial(rest_kernel, n_last),
        [img] * n_last,
        [*t_parts[:2], *kept],
        dims,
        n_last,
        3,
    )
    return dimgs + list(g), send, own


def pack_kernel(lab_hbm, img_hbm, out_ref, lab_scr, img_scr, sems):
    ni, nb, d = img_scr.shape
    bring = [
        pltpu.make_async_copy(img_hbm, img_scr, sems.at[0]),
        pltpu.make_async_copy(lab_hbm, lab_scr, sems.at[1]),
    ]
    for copy in bring:
        copy.start()
    for copy in bring:
        copy.wait()
    for i in range(ni):
        out_ref[i * nb : (i + 1) * nb, :] = img_scr[i]
    across = lax.broadcasted_iota(jnp.int32, (nb, nb), 0)
    along = lax.broadcasted_iota(jnp.int32, (nb, nb), 1)
    lab = jnp.broadcast_to(lab_scr[...].astype(F32), (nb, nb))
    lab = jnp.sum(jnp.where(across == along, lab, 0.0), axis=1, keepdims=True)
    out_ref[ni * nb :, :] = jnp.broadcast_to(lab, (nb, d))


def pack(images, labels):
    ni, nb, d = images.shape
    return pl.pallas_call(
        pack_kernel,
        out_shape=jax.ShapeDtypeStruct((ni * nb + nb, d), F32),
        in_specs=[pl.BlockSpec(memory_space=pltpu.HBM)] * 2,
        out_specs=pl.BlockSpec(memory_space=pltpu.VMEM),
        scratch_shapes=[
            pltpu.VMEM((1, nb), jnp.int32),
            pltpu.VMEM((ni, nb, d), F32),
            pltpu.SemaphoreType.DMA((2,)),
        ],
        compiler_params=pltpu.CompilerParams(vmem_limit_bytes=8 * MIB),
    )(stay(labels.reshape(1, nb)), stay(images))


def turn_kernel(nt, text_hbm, out_ref, *refs):
    *scrs, sems = refs
    half = scrs[0].shape[0] // nt
    bring = [
        pltpu.make_async_copy(
            text_hbm.at[:, pl.ds(128 * k, 128)], scr, sems.at[k]
        )
        for k, scr in enumerate(scrs)
    ]
    for copy in bring:
        copy.start()
    for k, scr in enumerate(scrs):
        bring[k].wait()
        for j in range(nt):
            out_ref[j * half : (j + 1) * half, 128 * k : 128 * (k + 1)] = scr[
                pl.ds(j, half, stride=nt), :
            ]


def turn(texts, nt):
    rows, d = texts.shape
    return pl.pallas_call(
        functools.partial(turn_kernel, nt),
        out_shape=jax.ShapeDtypeStruct((rows, d), F32),
        in_specs=[pl.BlockSpec(memory_space=pltpu.HBM)],
        out_specs=pl.BlockSpec(memory_space=pltpu.VMEM),
        scratch_shapes=[pltpu.VMEM((rows, 128), F32)] * (d // 128)
        + [pltpu.SemaphoreType.DMA((d // 128,))],
        compiler_params=pltpu.CompilerParams(vmem_limit_bytes=8 * MIB),
    )(stay(texts))


def sum_kernel(n, *refs):
    out_ref = refs[n]
    ni, nb, _ = out_ref.shape
    for i in range(ni):
        at = slice(i * nb, (i + 1) * nb)
        out_ref[i] = tree_sum([ref[at, :] for ref in refs[:n]])


def sum_pieces(pieces, ni, nb):
    d = pieces[0].shape[1]
    return pl.pallas_call(
        functools.partial(sum_kernel, len(pieces)),
        out_shape=jax.ShapeDtypeStruct((ni, nb, d), F32),
        in_specs=specs(len(pieces)),
        out_specs=specs(1)[0],
        compiler_params=pltpu.CompilerParams(vmem_limit_bytes=16 * MIB),
    )(*pieces)


def merge_kernel(n, own_ref, recv_ref, *outs):
    rows = outs[0].shape[0]
    grp = lax.axis_index("grp")
    for k, ref in enumerate(outs[:n]):
        at = pl.ds(pl.multiple_of((grp ^ k) * rows, 8), rows)
        ref[...] = own_ref[at, :] + recv_ref[at, :]
    outs[n][...] = own_ref[n * rows :, :] + recv_ref[n * rows :, :]


def merge(own, recv, n):
    rows = (own.shape[0] - 8) // n
    return pl.pallas_call(
        functools.partial(merge_kernel, n),
        out_shape=(jax.ShapeDtypeStruct((rows, 128), F32),) * n
        + (jax.ShapeDtypeStruct((8, 128), F32),),
        in_specs=specs(2),
        out_specs=tuple(specs(n + 1)),
        compiler_params=pltpu.CompilerParams(vmem_limit_bytes=16 * MIB),
    )(own, recv)


def total_kernel(n, *refs):
    out_ref = refs[-1]
    rows = refs[0].shape[0]
    out_ref[:rows, :] = tree_sum([ref[...] for ref in refs[:n]])
    out_ref[rows:, :] = tree_sum([ref[...] for ref in refs[n:-1]])


def total_of(parts, losses):
    rows = parts[0].shape[0]
    return pl.pallas_call(
        functools.partial(total_kernel, len(parts)),
        out_shape=jax.ShapeDtypeStruct((rows + 8, 128), F32),
        in_specs=specs(len(parts) + len(losses)),
        out_specs=specs(1)[0],
        compiler_params=pltpu.CompilerParams(vmem_limit_bytes=16 * MIB),
    )(*parts, *losses)


def place_kernel(n, count, *refs):
    ranks, (out_ref, loss_ref) = refs[:n], refs[n:]
    nc, nt, d = out_ref.shape
    lanes = d // 128
    units = nt // 8 * lanes // n
    grp = lax.axis_index("grp")
    for s in range(n):
        for i in range(units):
            unit = (grp ^ s) * units + i
            row = pl.multiple_of(8 * (unit // lanes), 8)
            lane = pl.multiple_of(128 * (unit % lanes), 128)
            for c in range(nc):
                out_ref[c, pl.ds(row, 8), pl.ds(lane, 128)] = ranks[s][
                    pl.ds(8 * nc * i + c, 8, stride=nc), :
                ]
    loss = tree_sum([ref[ref.shape[0] - 8 :, :] for ref in ranks])
    loss = jnp.sum(jnp.sum(loss, axis=1, keepdims=True), axis=0, keepdims=True)
    loss_ref[...] = loss / count


def place(ranks, shape, count):
    text_grads, loss = pl.pallas_call(
        functools.partial(place_kernel, len(ranks), float(count)),
        out_shape=(jax.ShapeDtypeStruct(shape, F32), jax.ShapeDtypeStruct((1, 1), F32)),
        in_specs=specs(len(ranks)),
        out_specs=tuple(specs(2)),
        compiler_params=pltpu.CompilerParams(vmem_limit_bytes=16 * MIB),
    )(*ranks)
    return text_grads, loss.reshape(())


def steps(image_tokens, text_tokens, labels):
    nb, ni, d = image_tokens.shape
    nc, nt, _ = text_tokens.shape
    n_blk, n_grp = lax.axis_size("blk"), lax.axis_size("grp")
    count = nb * n_blk * n_grp
    dims = (ni, nb, nt, 2 * nc, d)
    blk = lax.axis_index("blk")
    far = FAR(n_blk)
    order = grp_order(n_grp)

    mine = pack(jnp.transpose(image_tokens, (1, 0, 2)), labels)
    texts = text_tokens.reshape(nc * nt, d)
    imgs = [mine] + [swap(mine, "blk", k) for k in far]
    other = swap(texts, "blk", 1)
    own = turn(texts, nt)
    lane = lax.broadcasted_iota(jnp.int32, (8, 128), 1) % (2 * nc)
    text_ids = lane % nc + nc * jnp.where(lane < nc, blk ^ 1, blk)

    grads, send, own_part = compute(dims, text_ids, imgs, other, own)

    *parts, loss = merge(own_part, swap(send, "blk", 1), n_grp)
    arrived = {k: swap(parts[k], "grp", k) for k in order}
    losses = [loss] + [swap(loss, "blk", k) for k in sorted(far)]
    total = total_of(
        [parts[0]] + [arrived[k] for k in range(1, n_grp)], losses
    )
    got = {k: swap(total, "grp", k) for k in order}
    text_grads, loss = place(
        [total] + [got[k] for k in range(1, n_grp)], (nc, nt, d), count
    )

    grads = grads[:1] + [swap(g, "blk", k) for k, g in zip(far, grads[1:])]
    image_grads = jnp.transpose(sum_pieces(grads, ni, nb), (1, 0, 2))

    return loss, image_grads, text_grads


def grp_order(n_grp):
    return ORDER(n_grp)


def solution(mesh):
    placed = (P(("blk", "grp"), None, None), P("blk", None, None), P(("blk", "grp")))
    return jax.shard_map(
        steps,
        mesh=mesh,
        in_specs=placed,
        out_specs=(P(), P(("blk", "grp"), None, None), P("blk", None, None)),
        check_vma=False,
    )
```

```python
import functools

import jax
import jax.numpy as jnp
from jax import lax
from jax.experimental import pallas as pl
from jax.experimental.pallas import tpu as pltpu
from jax.sharding import PartitionSpec as P


F32 = jnp.float32
BF16 = jnp.bfloat16
LOW = -1e30
LOG2E = 1.4426950408889634
LN2 = 0.6931471805599453
MIB = 1024 * 1024


def FAR(n):
    first = [k for k in [6,2,4] if k < n]
    return first + [k for k in range(2, n, 2) if k not in first]


def swap(x, axis, k):
    n = lax.axis_size(axis)
    return lax.ppermute(x, axis, [(i, i ^ k) for i in range(n)])


def tree_sum(values):
    while len(values) > 1:
        values = [a + b for a, b in zip(values[::2], values[1::2])]
    return values[0]


def split(x, parts):
    out = []
    for p in range(parts):
        h = x.astype(BF16)
        out.append(h)
        if p + 1 < parts:
            x = x - h.astype(F32)
    return out


def dot_nt(a, b):
    return lax.dot_general(a, b, (((1,), (1,)), ((), ())), preferred_element_type=F32)


def dot_nn(a, b):
    return lax.dot_general(a, b, (((1,), (0,)), ((), ())), preferred_element_type=F32)


def lane_all(x, op, step):
    while step < 128:
        x = op(x, pltpu.roll(x, step, 1))
        step *= 2
    return x


def sublane_all(x, op, step):
    while step < 8:
        x = op(x, pltpu.roll(x, step, 0))
        step *= 2
    return x


def stay(x):
    return pltpu.with_memory_space_constraint(x, pltpu.HBM)


def specs(n):
    return [pl.BlockSpec(memory_space=pltpu.VMEM)] * n


def scores_of(img, t_parts):
    ih, im, il = img
    th, tm, tl = t_parts
    return (
        dot_nt(ih, th)
        + (dot_nt(ih, tm) + dot_nt(im, th))
        + (dot_nt(im, tm) + dot_nt(ih, tl) + dot_nt(il, th))
    )


def pair_math(dims, s, lab, text):
    ni, nb, nt, nc, _ = dims
    rows, (rp, width) = ni * nb, s.shape
    tiles = rp // 8
    pad = lax.broadcasted_iota(jnp.int32, (8, 1), 0) >= rows - 8 * (tiles - 1)

    def on_last(x, fill):
        if rp == rows:
            return x
        return jnp.concatenate(
            [x[: tiles - 1], jnp.where(pad, fill, x[tiles - 1])[None]], axis=0
        )

    cols = [
        on_last((s[:, k : k + 128] * LOG2E).reshape(tiles, 8, 128), LOW)
        for k in range(0, width, 128)
    ]

    def over_lanes(x, op):
        return lane_all(x.reshape(rp, 128), op, nc).reshape(tiles, 8, 128)

    row_max = over_lanes(functools.reduce(jnp.maximum, cols), jnp.maximum)
    col_max = [sublane_all(jnp.max(x, axis=0), jnp.maximum, nb) for x in cols]
    row_exp = [jnp.exp2(x - row_max) for x in cols]
    row_sum = over_lanes(functools.reduce(jnp.add, row_exp), jnp.add)
    col_exp = [jnp.exp2(x - m[None]) for x, m in zip(cols, col_max)]
    col_sum = [sublane_all(jnp.sum(x, axis=0), jnp.add, nb) for x in col_exp]
    image_pool = on_last(row_max * LN2 + jnp.log(row_sum), 0.0)
    image_pool = sublane_all(jnp.sum(image_pool, axis=0), jnp.add, nb) * (1.0 / ni)
    text_pool = functools.reduce(
        jnp.add, [m * LN2 + jnp.log(z) for m, z in zip(col_max, col_sum)]
    )
    text_pool = lane_all(text_pool, jnp.add, nc) * (1.0 / nt)
    logit = 4.0 * (0.5 * (image_pool + text_pool)) - 20.0
    sign = jnp.where(lab == text, 1.0, -1.0)
    z = -sign * logit
    e = jnp.exp(-jnp.abs(z))
    loss = jnp.maximum(z, 0.0) + jnp.log1p(e)
    dpair = -2.0 * sign * (jnp.where(z >= 0.0, 1.0, e) / (1.0 + e))
    row_w = on_last(((0.5 / ni) * dpair)[None] / row_sum, 0.0)
    ds = [
        (re * row_w + ce * ((0.5 / nt) * dpair / cz)[None]).reshape(rp, 128)
        for re, ce, cz in zip(row_exp, col_exp, col_sum)
    ]
    return jnp.concatenate(ds, axis=1), loss * (1.0 / ((8 // nb) * (128 // nc)))


def label_tile(img_ref, nb):
    rp = img_ref.shape[0]
    tail = img_ref[rp - 8 :, :128]
    sub = lax.broadcasted_iota(jnp.int32, (8, 128), 0)
    return jnp.where(sub >= 8 - nb, tail, pltpu.roll(tail, nb, 0)).astype(jnp.int32)


def image_grad(w, t_parts):
    wh, wl = w
    th, tm, _ = t_parts
    return dot_nn(wh, th) + (dot_nn(wh, tm) + dot_nn(wl, th))


def text_grad(turned_img, w):
    (ith, itl), (wh, wl) = turned_img, w
    return dot_nn(ith, wh) + (dot_nn(ith, wl) + dot_nn(itl, wh))


def weights_of(dims, imgs, t_parts, text):
    scores, turned, out, losses = [], [], [], []
    for ref in imgs:
        img = ref[...]
        turned.append(split(img.T, 2))
        scores.append(scores_of(split(img, 3), t_parts))
    for ref, s in zip(imgs, scores):
        ds, loss = pair_math(dims, s, label_tile(ref, dims[1]), text)
        out.append(split(ds, 2))
        losses.append(loss)
    return turned, out, functools.reduce(jnp.add, losses)


def first_kernel(dims, ids_ref, img_ref, other_ref, own_ref, *refs):
    _, _, nt, nc, _ = dims
    half = nc // 2
    dimg_ref, acc_ref, loss_ref, *t_refs = refs[:6]
    scrs = refs[6:]
    for k, scr in enumerate(scrs):
        scr[...] = other_ref[:, 128 * k : 128 * (k + 1)]
    text = jnp.concatenate(
        [
            jnp.concatenate(
                [
                    x
                    for j in range(nt)
                    for x in (
                        scr[pl.ds(j, half, stride=nt), :],
                        own_ref[j * half : (j + 1) * half, 128 * k : 128 * (k + 1)],
                    )
                ],
                axis=0,
            )
            for k, scr in enumerate(scrs)
        ],
        axis=1,
    )
    for ref, x in zip(t_refs, split(text, 3)):
        ref[...] = x
    tp = [ref[...] for ref in t_refs]
    turned, w, loss = weights_of(dims, [img_ref], tp, ids_ref[...])
    loss_ref[...] = loss
    dimg_ref[...] = image_grad(w[0], tp)
    acc_ref[...] = text_grad(turned[0], w[0])


def middle_kernel(dims, n, ids_ref, *refs):
    imgs, (acc_in, loss_in, *t_refs) = refs[:n], refs[n : n + 5]
    dimgs, (acc_ref, loss_ref) = refs[n + 5 : 2 * n + 5], refs[2 * n + 5 :]
    tp = [ref[...] for ref in t_refs]
    turned, w, loss = weights_of(dims, imgs, tp, ids_ref[...])
    loss_ref[...] = loss_in[...] + loss
    acc = acc_in[...]
    for p in range(n):
        dimgs[p][...] = image_grad(w[p], tp)
        acc = acc + text_grad(turned[p], w[p])
    acc_ref[...] = acc


def hand_out(dims, turned, send_ref, own_ref):
    nt, nc, d = dims[2:]
    half = nc // 2
    for j in range(nt):
        g, q = divmod(j, 8)
        for k in range(d // 128):
            to = ((g * (d // 128) + k) * 8 + q) * half
            for h, ref in enumerate((send_ref, own_ref)):
                ref[to : to + half, :] = turned[
                    j * nc + h * half : j * nc + (h + 1) * half,
                    128 * k : 128 * (k + 1),
                ]


def last_kernel(dims, n, ids_ref, *refs):
    imgs, (acc_in, loss_in, *t_refs) = refs[:n], refs[n : n + 5]
    send_ref, own_ref, *keep = refs[n + 5 :]
    tp = [ref[...] for ref in t_refs]
    turned, w, loss = weights_of(dims, imgs, tp, ids_ref[...])
    acc = acc_in[...]
    for p in range(n):
        acc = acc + text_grad(turned[p], w[p])
        for ref, x in zip(keep[2 * p : 2 * p + 2], w[p]):
            ref[...] = x
    hand_out(dims, acc.T, send_ref, own_ref)
    for ref in (send_ref, own_ref):
        ref[ref.shape[0] - 8 :, :] = loss_in[...] + loss


def rest_kernel(n, th_ref, tm_ref, *refs):
    tp = (th_ref[...], tm_ref[...], None)
    for p in range(n):
        w = [ref[...] for ref in refs[2 * p : 2 * p + 2]]
        refs[2 * n + p][...] = image_grad(w, tp)


def call(kernel, outs, args, dims, n, mats, scratch=(), limit=48):
    ni, nb, nt, nc, d = dims
    return pl.pallas_call(
        kernel,
        out_shape=tuple(jax.ShapeDtypeStruct(*o) for o in outs),
        in_specs=specs(len(args)),
        out_specs=tuple(specs(len(outs))),
        scratch_shapes=list(scratch),
        cost_estimate=pl.CostEstimate(
            flops=2 * ni * nb * nt * nc * d * mats * n,
            bytes_accessed=4 * nt * nc * d,
            transcendentals=2 * ni * nb * nt * nc * n,
        ),
        compiler_params=pltpu.CompilerParams(vmem_limit_bytes=limit * MIB),
    )(*args)


def compute(dims, ids, imgs, other, own):
    ni, nb, nt, nc, d = dims
    width = nt * nc
    rp = ni * nb + nb
    part = (nt * nc * d // 2 // 128 + 8, 128)
    img, acc, loss = ((rp, d), F32), ((d, width), F32), ((8, 128), F32)
    keep = [((rp, width), BF16)] * 2
    dimgs = []
    out = call(
        functools.partial(first_kernel, dims),
        [img, acc, loss] + [((width, d), BF16)] * 3,
        [ids, imgs[0], other, own],
        dims,
        1,
        12,
        [pltpu.VMEM((width // 2, 128), F32)] * (d // 128),
    )
    dimgs.append(out[0])
    state, t_parts = out[1:3], out[3:]
    n_last = 2 if len(imgs) > 2 else 1
    for p in range(1, len(imgs) - n_last):
        *g, a, b = call(
            functools.partial(middle_kernel, dims, 1),
            [img, acc, loss],
            [ids, imgs[p], *state, *t_parts],
            dims,
            1,
            12,
        )
        dimgs += g
        state = (a, b)
    send, own, *kept = call(
        functools.partial(last_kernel, dims, n_last),
        [(part, F32)] * 2 + keep * n_last,
        [ids, *imgs[-n_last:], *state, *t_parts],
        dims,
        n_last,
        9,
    )
    g = call(
        functools.partial(rest_kernel, n_last),
        [img] * n_last,
        [*t_parts[:2], *kept],
        dims,
        n_last,
        3,
    )
    return dimgs + list(g), send, own


def pack_kernel(lab_hbm, img_hbm, out_ref, lab_scr, img_scr, sems):
    ni, nb, d = img_scr.shape
    bring = [
        pltpu.make_async_copy(img_hbm, img_scr, sems.at[0]),
        pltpu.make_async_copy(lab_hbm, lab_scr, sems.at[1]),
    ]
    for copy in bring:
        copy.start()
    for copy in bring:
        copy.wait()
    for i in range(ni):
        out_ref[i * nb : (i + 1) * nb, :] = img_scr[i]
    across = lax.broadcasted_iota(jnp.int32, (nb, nb), 0)
    along = lax.broadcasted_iota(jnp.int32, (nb, nb), 1)
    lab = jnp.broadcast_to(lab_scr[...].astype(F32), (nb, nb))
    lab = jnp.sum(jnp.where(across == along, lab, 0.0), axis=1, keepdims=True)
    out_ref[ni * nb :, :] = jnp.broadcast_to(lab, (nb, d))


def pack(images, labels):
    ni, nb, d = images.shape
    return pl.pallas_call(
        pack_kernel,
        out_shape=jax.ShapeDtypeStruct((ni * nb + nb, d), F32),
        in_specs=[pl.BlockSpec(memory_space=pltpu.HBM)] * 2,
        out_specs=pl.BlockSpec(memory_space=pltpu.VMEM),
        scratch_shapes=[
            pltpu.VMEM((1, nb), jnp.int32),
            pltpu.VMEM((ni, nb, d), F32),
            pltpu.SemaphoreType.DMA((2,)),
        ],
        compiler_params=pltpu.CompilerParams(vmem_limit_bytes=8 * MIB),
    )(stay(labels.reshape(1, nb)), stay(images))


def turn_kernel(nt, text_hbm, out_ref, *refs):
    *scrs, sems = refs
    half = scrs[0].shape[0] // nt
    bring = [
        pltpu.make_async_copy(
            text_hbm.at[:, pl.ds(128 * k, 128)], scr, sems.at[k]
        )
        for k, scr in enumerate(scrs)
    ]
    for copy in bring:
        copy.start()
    for k, scr in enumerate(scrs):
        bring[k].wait()
        for j in range(nt):
            out_ref[j * half : (j + 1) * half, 128 * k : 128 * (k + 1)] = scr[
                pl.ds(j, half, stride=nt), :
            ]


def turn(texts, nt):
    rows, d = texts.shape
    return pl.pallas_call(
        functools.partial(turn_kernel, nt),
        out_shape=jax.ShapeDtypeStruct((rows, d), F32),
        in_specs=[pl.BlockSpec(memory_space=pltpu.HBM)],
        out_specs=pl.BlockSpec(memory_space=pltpu.VMEM),
        scratch_shapes=[pltpu.VMEM((rows, 128), F32)] * (d // 128)
        + [pltpu.SemaphoreType.DMA((d // 128,))],
        compiler_params=pltpu.CompilerParams(vmem_limit_bytes=8 * MIB),
    )(stay(texts))


def sum_kernel(n, *refs):
    out_ref = refs[n]
    ni, nb, _ = out_ref.shape
    for i in range(ni):
        at = slice(i * nb, (i + 1) * nb)
        out_ref[i] = tree_sum([ref[at, :] for ref in refs[:n]])


def sum_pieces(pieces, ni, nb):
    d = pieces[0].shape[1]
    return pl.pallas_call(
        functools.partial(sum_kernel, len(pieces)),
        out_shape=jax.ShapeDtypeStruct((ni, nb, d), F32),
        in_specs=specs(len(pieces)),
        out_specs=specs(1)[0],
        compiler_params=pltpu.CompilerParams(vmem_limit_bytes=16 * MIB),
    )(*pieces)


def merge_kernel(n, own_ref, recv_ref, *outs):
    rows = outs[0].shape[0]
    grp = lax.axis_index("grp")
    for k, ref in enumerate(outs[:n]):
        at = pl.ds(pl.multiple_of((grp ^ k) * rows, 8), rows)
        ref[...] = own_ref[at, :] + recv_ref[at, :]
    outs[n][...] = own_ref[n * rows :, :] + recv_ref[n * rows :, :]


def merge(own, recv, n):
    rows = (own.shape[0] - 8) // n
    return pl.pallas_call(
        functools.partial(merge_kernel, n),
        out_shape=(jax.ShapeDtypeStruct((rows, 128), F32),) * n
        + (jax.ShapeDtypeStruct((8, 128), F32),),
        in_specs=specs(2),
        out_specs=tuple(specs(n + 1)),
        compiler_params=pltpu.CompilerParams(vmem_limit_bytes=16 * MIB),
    )(own, recv)


def total_kernel(n, *refs):
    out_ref = refs[-1]
    rows = refs[0].shape[0]
    out_ref[:rows, :] = tree_sum([ref[...] for ref in refs[:n]])
    out_ref[rows:, :] = tree_sum([ref[...] for ref in refs[n:-1]])


def total_of(parts, losses):
    rows = parts[0].shape[0]
    return pl.pallas_call(
        functools.partial(total_kernel, len(parts)),
        out_shape=jax.ShapeDtypeStruct((rows + 8, 128), F32),
        in_specs=specs(len(parts) + len(losses)),
        out_specs=specs(1)[0],
        compiler_params=pltpu.CompilerParams(vmem_limit_bytes=16 * MIB),
    )(*parts, *losses)


def place_kernel(n, count, *refs):
    ranks, (out_ref, loss_ref) = refs[:n], refs[n:]
    nc, nt, d = out_ref.shape
    lanes = d // 128
    units = nt // 8 * lanes // n
    grp = lax.axis_index("grp")
    for s in range(n):
        for i in range(units):
            unit = (grp ^ s) * units + i
            row = pl.multiple_of(8 * (unit // lanes), 8)
            lane = pl.multiple_of(128 * (unit % lanes), 128)
            for c in range(nc):
                out_ref[c, pl.ds(row, 8), pl.ds(lane, 128)] = ranks[s][
                    pl.ds(8 * nc * i + c, 8, stride=nc), :
                ]
    loss = tree_sum([ref[ref.shape[0] - 8 :, :] for ref in ranks])
    loss = jnp.sum(jnp.sum(loss, axis=1, keepdims=True), axis=0, keepdims=True)
    loss_ref[...] = loss / count


def place(ranks, shape, count):
    text_grads, loss = pl.pallas_call(
        functools.partial(place_kernel, len(ranks), float(count)),
        out_shape=(jax.ShapeDtypeStruct(shape, F32), jax.ShapeDtypeStruct((1, 1), F32)),
        in_specs=specs(len(ranks)),
        out_specs=tuple(specs(2)),
        compiler_params=pltpu.CompilerParams(vmem_limit_bytes=16 * MIB),
    )(*ranks)
    return text_grads, loss.reshape(())


def steps(image_tokens, text_tokens, labels):
    nb, ni, d = image_tokens.shape
    nc, nt, _ = text_tokens.shape
    n_blk, n_grp = lax.axis_size("blk"), lax.axis_size("grp")
    count = nb * n_blk * n_grp
    dims = (ni, nb, nt, 2 * nc, d)
    blk = lax.axis_index("blk")
    far = FAR(n_blk)
    order = grp_order(n_grp)

    mine = pack(jnp.transpose(image_tokens, (1, 0, 2)), labels)
    texts = text_tokens.reshape(nc * nt, d)
    imgs = [mine] + [swap(mine, "blk", k) for k in far]
    other = swap(texts, "blk", 1)
    own = turn(texts, nt)
    lane = lax.broadcasted_iota(jnp.int32, (8, 128), 1) % (2 * nc)
    text_ids = lane % nc + nc * jnp.where(lane < nc, blk ^ 1, blk)

    grads, send, own_part = compute(dims, text_ids, imgs, other, own)

    *parts, loss = merge(own_part, swap(send, "blk", 1), n_grp)
    arrived = {k: swap(parts[k], "grp", k) for k in order}
    losses = [loss] + [swap(loss, "blk", k) for k in sorted(far)]
    total = total_of(
        [parts[0]] + [arrived[k] for k in range(1, n_grp)], losses
    )
    got = {k: swap(total, "grp", k) for k in order}
    text_grads, loss = place(
        [total] + [got[k] for k in range(1, n_grp)], (nc, nt, d), count
    )

    grads = grads[:1] + [swap(g, "blk", k) for k, g in zip(far, grads[1:])]
    image_grads = jnp.transpose(sum_pieces(grads, ni, nb), (1, 0, 2))

    return loss, image_grads, text_grads


def grp_order(n_grp):
    return list(range(n_grp - 1, 0, -1))


def solution(mesh):
    placed = (P(("blk", "grp"), None, None), P("blk", None, None), P(("blk", "grp")))
    return jax.shard_map(
        steps,
        mesh=mesh,
        in_specs=placed,
        out_specs=(P(), P(("blk", "grp"), None, None), P("blk", None, None)),
        check_vma=False,
    )
```
